32 devices in a mesh: kpt: 2 (over y), ga: 16 (over z, x, core).
Axes of the slice: x: 2, y: 2, z: 4, core: 2. Of those that a mesh axis runs over, the one named last changes fastest.
Arguments:
- miller_index: int32 [3, 12288], P(None, 'ga'), may hold values from -12 to 12
- kpoint: float32 [6], P('kpt'), parts along dimension 0, may hold values from -0.5 to 0.5
- waves: bfloat16 [2, 256, 12288], P(None, 'kpt', 'ga'), parts along dimension 1, may hold values from -6 to 6
- species: int32 [16], replicated, may hold values from 0 to 3
- counts: int32 [16], replicated, may hold values from 1 to 8
- positions: int32 [3, 16], replicated, may hold values from 0 to 63
- radial_coef: float32 [4, 8, 16], replicated, may hold values from -4 to 4
- coupling: float32 [16, 8, 8], replicated, as said below
Outputs:
- applied: bfloat16 [2, 256, 12288], P(None, 'kpt', 'ga'), parts along dimension 1
- energy: float32 [256], P('kpt'), parts along dimension 0
The draws below stay inside these ranges and needn't reach their ends.
There are 2 independent parts, one for each index of `kpt`. The reference program is written for one: setup_inputs(seed, part) draws one part's arguments, and reference() takes and returns one part's arrays. A program takes and returns all parts, laid end to end along the dimension named above; an argument that names none is the same for every part. Nothing has to cross between parts.
Inputs may be any that keep to these rules, and one draw needn't show every extreme that they name: `coupling`: symmetric in its last two dimensions.
All inputs are finite; a program needn't handle non-finite values.
Results may differ from the reference program's by a relative error of at most 0.0062.
Values may be sent and summed in bfloat16 or wider, within the bound.
A program may use at most 64 MiB of HBM per device.

```python
import math
import jax
import jax.numpy as jnp
from jax import lax

BANDS = 128
PROJ = 8
NSPEC = 4
NRAD = 16
MGRID = 64
HMAX = 12
ATOM_BLOCK = 16
NAT = 16
PW = 12288
NPROJ = 128
NBLK = 1


def draw_coupling(key, part):
    first, second, third = jax.random.split(key, 3)
    raw = jax.random.normal(first, (NAT, PROJ, PROJ), jnp.float32)
    symmetric = 0.6 * (raw + jnp.swapaxes(raw, 1, 2))
    diagonal = jax.random.uniform(second, (NAT, PROJ), jnp.float32, 3.0, 6.0)
    signs = jnp.where(jax.random.bernoulli(third, 0.7, (NAT, PROJ)), 1.0, -1.0)
    return symmetric + jnp.eye(PROJ, dtype=jnp.float32)[None] * (diagonal * signs)[:, :, None]


def touch_ends(values, key, low, high):
    dims = values.shape
    index_at = [jax.random.randint(jax.random.fold_in(key, axis), (), 0, dims[axis]) for axis in range(len(dims))]
    values = values.at[tuple(index_at)].set(low)
    longest = dims.index(max(dims))
    index_at[longest] = (index_at[longest] + 1) % dims[longest]
    return values.at[tuple(index_at)].set(high)


def level_of(stream_key, dims, shards, least, top_value):
    loudness, own = 1.0, jax.random.fold_in(stream_key, 6)
    for position, parts in shards:
        steps = jnp.exp(jax.random.uniform(jax.random.fold_in(own, position), (parts,), jnp.float32, least / len(shards), top_value / len(shards)))
        loudness = loudness * jnp.repeat(steps, dims[position] // parts).reshape([-1 if axis == position else 1 for axis in range(len(dims))])
    return loudness


def normal_values(stream_key, extent, deviation, bound, shards=(), kind=jnp.bfloat16):
    values = deviation * jax.random.normal(stream_key, extent, jnp.float32)
    if shards:
        values = values * level_of(stream_key, extent, shards, -0.22, 0.18)
    return jnp.clip(values, -bound, bound).astype(kind)


def setup_inputs(seed: int = 0, part: int = 0) -> dict:
    splits = jax.random.split(jax.random.key(seed), 9)
    part_splits = jax.random.split(jax.random.fold_in(splits[8], part), 9)
    miller_index = touch_ends(jax.random.randint(splits[0], (3, PW), -HMAX, HMAX + 1), jax.random.fold_in(splits[0], 1), -HMAX, HMAX).astype(jnp.int32)
    kpoint = jnp.clip(jax.random.uniform(part_splits[1], (3,), jnp.float32, -0.5, 0.5), -0.5, 0.5)
    waves = normal_values(part_splits[2], (2, BANDS, PW), 1.0, 6.0, ((2, 16),))
    species = touch_ends(jax.random.randint(splits[3], (NAT,), 0, NSPEC), jax.random.fold_in(splits[3], 1), 0, NSPEC - 1).astype(jnp.int32)
    counts = touch_ends(jax.random.randint(splits[4], (NAT,), 1, PROJ + 1), jax.random.fold_in(splits[4], 1), 1, PROJ).astype(jnp.int32)
    positions = touch_ends(jax.random.randint(splits[5], (3, NAT), 0, MGRID), jax.random.fold_in(splits[5], 1), 0, MGRID - 1).astype(jnp.int32)
    radial_coef = normal_values(splits[6], (NSPEC, PROJ, NRAD), 1.0, 4.0, (), jnp.float32)
    coupling = draw_coupling(jax.random.fold_in(splits[8], 71), part)
    return dict(miller_index=miller_index, kpoint=kpoint, waves=waves, species=species, counts=counts, positions=positions, radial_coef=radial_coef, coupling=coupling)


def prepare(miller_index, kpoint, terms):
    shifted = miller_index.astype(jnp.float32) + kpoint[:, None]
    squared = lax.optimization_barrier(jnp.sum(shifted * shifted, axis=0))
    widths = 0.001 * 1.5 ** jnp.arange(terms).astype(jnp.float32)
    basis = jnp.exp(-widths[:, None] * squared[None, :])
    angular = jnp.concatenate([jnp.ones_like(squared)[None], shifted / jnp.sqrt(squared + 1.0)[None]], 0)
    angular = jnp.concatenate([angular, angular], 0)
    return (basis, angular)

def projectors(first, miller_index, kpoint, basis, angular, species, counts, positions, radial_coef, scaling):
    kinds = lax.dynamic_slice_in_dim(species, first, ATOM_BLOCK)
    numbers = lax.dynamic_slice_in_dim(counts, first, ATOM_BLOCK)
    places = lax.dynamic_slice_in_dim(positions, first, ATOM_BLOCK, 1)
    selector = (kinds[:, None] == jnp.arange(radial_coef.shape[0]).astype(jnp.int32)[None, :]).astype(jnp.float32)
    chosen = jnp.einsum('as,sjr->ajr', selector, radial_coef, precision=lax.Precision.HIGHEST)
    radial = jnp.einsum('ajr,rg->ajg', chosen, basis, precision=lax.Precision.HIGHEST)
    active = (jnp.arange(PROJ).astype(jnp.int32)[None, :] < numbers[:, None]).astype(jnp.float32)
    amplitude = radial * angular[None] * active[:, :, None] * scaling
    winding = jnp.mod(lax.optimization_barrier(jnp.sum(miller_index[:, None, :] * places[:, :, None], axis=0)), MGRID)
    offset = lax.optimization_barrier(jnp.sum(kpoint[:, None] * places.astype(jnp.float32), axis=0))
    phase = 2.0 * math.pi / MGRID * (winding.astype(jnp.float32) + offset[:, None])
    planes = miller_index.shape[1]
    real_part = (amplitude * jnp.cos(phase)[:, None, :]).astype(jnp.bfloat16).reshape(ATOM_BLOCK * PROJ, planes)
    imag_part = (-amplitude * jnp.sin(phase)[:, None, :]).astype(jnp.bfloat16).reshape(ATOM_BLOCK * PROJ, planes)
    return (real_part, imag_part)

def reference(miller_index, kpoint, waves, species, counts, positions, radial_coef, coupling):
    scaling = 1.0 / math.sqrt(PW)
    basis, angular = prepare(miller_index, kpoint, radial_coef.shape[2])
    wave_re = waves[0].astype(jnp.float32)
    wave_im = waves[1].astype(jnp.float32)
    width = ATOM_BLOCK * PROJ

    def build(index):
        return projectors(index * ATOM_BLOCK, miller_index, kpoint, basis, angular, species, counts, positions, radial_coef, scaling)

    def measure(index):
        real_part, imag_part = build(index)
        real_part = real_part.astype(jnp.float32)
        imag_part = imag_part.astype(jnp.float32)
        over_re = jnp.einsum('sg,bg->sb', real_part, wave_re) + jnp.einsum('sg,bg->sb', imag_part, wave_im)
        over_im = jnp.einsum('sg,bg->sb', real_part, wave_im) - jnp.einsum('sg,bg->sb', imag_part, wave_re)
        return jnp.stack([over_re, over_im])
    table = lax.map(measure, jnp.arange(NBLK).astype(jnp.int32))
    table = jnp.transpose(table, (1, 0, 2, 3)).reshape(2, NAT, PROJ, BANDS)
    weighted = jnp.einsum('aij,cajb->caib', coupling, table, precision=lax.Precision.HIGHEST)
    energy = lax.optimization_barrier(jnp.sum(table * weighted, axis=(0, 1, 2))) / NPROJ
    rounded = weighted.reshape(2, NPROJ, BANDS).astype(jnp.bfloat16)

    def accumulate(total, index):
        real_part, imag_part = build(index)
        real_part = real_part.astype(jnp.float32)
        imag_part = imag_part.astype(jnp.float32)
        rows = lax.dynamic_slice_in_dim(rounded, (index * width).astype(jnp.int32), width, 1).astype(jnp.float32)
        out_re = jnp.einsum('sb,sg->bg', rows[0], real_part) - jnp.einsum('sb,sg->bg', rows[1], imag_part)
        out_im = jnp.einsum('sb,sg->bg', rows[1], real_part) + jnp.einsum('sb,sg->bg', rows[0], imag_part)
        return (total + jnp.stack([out_re, out_im]), None)
    output, unused = lax.scan(accumulate, jnp.zeros((2, BANDS, PW), jnp.float32), jnp.arange(NBLK).astype(jnp.int32))
    return (output.astype(jnp.bfloat16), energy)
```

```python
import functools
import math

import jax
import jax.numpy as jnp
import numpy as np
from jax import lax
from jax.experimental import pallas as pl
from jax.experimental.pallas import tpu as pltpu
from jax.sharding import PartitionSpec as P

PROJ = 8
MGRID = 64
ATOM_BLOCK = 16


def turn_polynomials(degree=8):
    nodes = 0.125 * (1.0 + np.cos(np.pi * (np.arange(200) + 0.5) / 200))
    root = np.sqrt(nodes)
    sine = np.polynomial.Chebyshev.fit(nodes, np.sin(2 * np.pi * root) / root, degree, domain=[0, 0.25])
    cosine = np.polynomial.Chebyshev.fit(nodes, np.cos(2 * np.pi * root), degree, domain=[0, 0.25])
    kind = np.polynomial.Polynomial
    return [[float(c) for c in p.convert(kind=kind).coef] for p in (sine, cosine)]


SINE, COSINE = turn_polynomials()


def horner(coefs, x):
    total = coefs[-1]
    for c in coefs[-2::-1]:
        total = total * x + c
    return total


def peers_of(me, n, body):
    if n <= 32:
        order = sorted(range(1, n), key=lambda k: -min(k, n - k))
        for k in order:
            body(lax.rem(me + k, n))
    else:
        lax.fori_loop(1, n, lambda k, c: (body(lax.rem(me + k, n)), c)[1], 0)


def loop(count, body):
    if count == 1:
        body(0)
    else:
        lax.fori_loop(0, count, lambda i, c: (body(i), c)[1], 0)


def kernel(
    n,
    scaling,
    miller_ref,
    kpoint_ref,
    waves_ref,
    species_ref,
    counts_ref,
    positions_ref,
    radial_ref,
    coupling_ref,
    out_ref,
    energy_ref,
    vbuf,
    bbuf,
    trig,
    table,
    part,
    send,
    recv,
    wbuf,
    ebuf,
    obuf,
    wave_sem,
    out_sem,
    send_sems,
    recv_sems,
):
    me = lax.axis_index("ga")
    atoms = coupling_ref.shape[2]
    own = atoms // n
    bands = waves_ref.shape[1]
    planes = waves_ref.shape[2]
    species_n, _, terms = radial_ref.shape
    f32 = jnp.float32

    wave_copy = pltpu.make_async_copy(waves_ref, vbuf, wave_sem)
    wave_copy.start()
    barrier = pltpu.get_barrier_semaphore()

    def greet(peer):
        pl.semaphore_signal(
            barrier, inc=1, device_id={"ga": peer}, device_id_type=pl.DeviceIdType.MESH
        )

    peers_of(me, n, greet)

    millers = [miller_ref[c : c + 1, :].astype(f32) for c in range(3)]
    shifted = [millers[c] + kpoint_ref[c] for c in range(3)]
    squared = shifted[0] * shifted[0] + shifted[1] * shifted[1] + shifted[2] * shifted[2]
    row = lax.broadcasted_iota(jnp.int32, (PROJ, planes), 0)
    inverse = 1.0 / jnp.sqrt(squared + 1.0)
    kind = lax.rem(row, 4)
    angular = jnp.full((PROJ, planes), scaling, f32)
    for c in range(3):
        angular = jnp.where(kind == c + 1, shifted[c] * inverse * scaling, angular)
    sums = [jnp.zeros((PROJ, planes), f32) for _ in range(species_n)]
    coefs = [radial_ref[s] for s in range(species_n)]
    for r in range(terms):
        width = float(np.float32(0.001) * np.float32(1.5) ** np.float32(r))
        basis = jnp.exp(-width * squared)
        for s in range(species_n):
            sums[s] = sums[s] + coefs[s][:, r : r + 1] * basis
    for s in range(species_n):
        table[s] = sums[s] * angular

    recv[pl.ds(me * own, own)] = jnp.zeros((own, 2 * PROJ, bands), recv.dtype)

    def build(block):
        first = block * ATOM_BLOCK
        diagonal = lax.broadcasted_iota(jnp.int32, (ATOM_BLOCK, atoms), 0) + first
        diagonal = diagonal == lax.broadcasted_iota(jnp.int32, (ATOM_BLOCK, atoms), 1)
        winding = jnp.zeros((ATOM_BLOCK, planes), f32)
        offset = jnp.zeros((ATOM_BLOCK, 1), f32)
        for c in range(3):
            places = positions_ref[c : c + 1, :].astype(f32)
            column = jnp.sum(jnp.where(diagonal, places, 0.0), axis=1, keepdims=True)
            winding = winding + column * millers[c]
            offset = offset + column * kpoint_ref[c]
        winding = winding - MGRID * jnp.floor(winding * (1.0 / MGRID))
        turns = (winding + offset) * (1.0 / MGRID)
        turns = turns - jnp.floor(turns + 0.5)
        square = turns * turns
        trig[0] = horner(COSINE, square)
        trig[1] = -(turns * horner(SINE, square))
        for a in range(ATOM_BLOCK):
            live = row < counts_ref[first + a]
            amplitude = jnp.where(live, table[species_ref[first + a]], 0.0)
            both = jnp.concatenate(
                [amplitude * trig[0, a : a + 1, :], amplitude * trig[1, a : a + 1, :]], axis=0
            )
            at = (first + a) * (2 * PROJ)
            if not isinstance(at, int):
                at = pl.multiple_of(at, 2 * PROJ)
            bbuf[pl.ds(at, 2 * PROJ), :] = both.astype(bbuf.dtype)

    loop(atoms // ATOM_BLOCK, build)
    wave_copy.wait()
    height = ATOM_BLOCK * 2 * PROJ

    def intersect(block):
        at = block * height
        if not isinstance(at, int):
            at = pl.multiple_of(at, height)
        product = lax.dot_general(
            bbuf[pl.ds(at, height), :],
            vbuf[...].reshape(2 * bands, planes),
            (((1,), (1,)), ((), ())),
            preferred_element_type=f32,
        )
        product = product.reshape(ATOM_BLOCK, 2, PROJ, 2 * bands)
        over_re = product[:, 0, :, :bands] + product[:, 1, :, bands:]
        over_im = product[:, 0, :, bands:] - product[:, 1, :, :bands]
        over = jnp.concatenate([over_re, over_im], axis=1)
        part[pl.ds(block * ATOM_BLOCK, ATOM_BLOCK)] = over
        send[pl.ds(block * ATOM_BLOCK, ATOM_BLOCK)] = over.astype(send.dtype)

    loop(atoms // ATOM_BLOCK, intersect)
    pl.semaphore_wait(barrier, n - 1)

    def scatter(peer):
        pltpu.make_async_remote_copy(
            src_ref=send.at[pl.ds(peer * own, own)],
            dst_ref=recv.at[pl.ds(me * own, own)],
            send_sem=send_sems.at[0],
            recv_sem=recv_sems.at[0],
            device_id={"ga": peer},
            device_id_type=pl.DeviceIdType.MESH,
        ).start()

    peers_of(me, n, scatter)

    columns = []
    for k in range(own):
        mine = lax.broadcasted_iota(jnp.int32, (PROJ, atoms), 1) == me * own + k
        columns.append(
            [
                jnp.broadcast_to(
                    jnp.sum(jnp.where(mine, coupling_ref[j], 0.0), axis=1, keepdims=True),
                    (PROJ, bands),
                )
                for j in range(PROJ)
            ]
        )

    def all_of(ref, sem):
        view = ref.at[pl.ds(0, ref.shape[0] // n * (n - 1))]
        return pltpu.make_async_copy(view, view, sem)

    all_of(recv, recv_sems.at[0]).wait()
    energy = jnp.zeros((1, bands), f32)
    for k in range(own):
        over = part[me * own + k]
        for p in range(n):
            over = over + recv[p * own + k].astype(f32)
        weighted = []
        for half in range(2):
            piece = over[half * PROJ : (half + 1) * PROJ]
            total = columns[k][0] * piece[0:1]
            for j in range(1, PROJ):
                total = total + columns[k][j] * piece[j : j + 1]
            energy = energy + jnp.sum(total * piece, axis=0, keepdims=True)
            weighted.append(total)
        wbuf[me * own + k] = jnp.concatenate(weighted, axis=0).astype(wbuf.dtype)
    ebuf[me] = energy

    def gather(peer):
        pltpu.make_async_remote_copy(
            src_ref=wbuf.at[pl.ds(me * own, own)],
            dst_ref=wbuf.at[pl.ds(me * own, own)],
            send_sem=send_sems.at[1],
            recv_sem=recv_sems.at[1],
            device_id={"ga": peer},
            device_id_type=pl.DeviceIdType.MESH,
        ).start()

    def gather_energy(peer):
        pltpu.make_async_remote_copy(
            src_ref=ebuf.at[me],
            dst_ref=ebuf.at[me],
            send_sem=send_sems.at[2],
            recv_sem=recv_sems.at[2],
            device_id={"ga": peer},
            device_id_type=pl.DeviceIdType.MESH,
        ).start()

    peers_of(me, n, gather)
    peers_of(me, n, gather_energy)
    all_of(send, send_sems.at[0]).wait()
    all_of(wbuf, recv_sems.at[1]).wait()

    weights = wbuf[...].astype(f32)
    upper, lower = weights[:, :PROJ], weights[:, PROJ:]
    halves = (
        jnp.concatenate([upper, -lower], axis=1),
        jnp.concatenate([lower, upper], axis=1),
    )
    copies = []
    for half in range(2):
        matrix = halves[half].astype(bbuf.dtype).reshape(atoms * 2 * PROJ, bands)
        obuf[half] = lax.dot_general(
            matrix, bbuf[...], (((0,), (0,)), ((), ())), preferred_element_type=f32
        ).astype(obuf.dtype)
        copies.append(pltpu.make_async_copy(obuf.at[half], out_ref.at[half], out_sem.at[half]))
        copies[-1].start()
    all_of(ebuf, recv_sems.at[2]).wait()
    energy_ref[...] = jnp.sum(ebuf[...], axis=(0, 1)) / (atoms * PROJ)
    all_of(wbuf, send_sems.at[1]).wait()
    all_of(ebuf, send_sems.at[2]).wait()
    for copy in copies:
        copy.wait()


def on_device(miller_index, kpoint, waves, species, counts, positions, radial_coef, coupling):
    n = lax.axis_size("ga")
    _, bands, planes = waves.shape
    atoms = coupling.shape[0]
    scaling = 1.0 / math.sqrt(planes * n)
    vmem = pl.BlockSpec(memory_space=pltpu.VMEM)
    smem = pl.BlockSpec(memory_space=pltpu.SMEM)
    anywhere = pl.BlockSpec(memory_space=pl.ANY)
    bf16, f32 = jnp.bfloat16, jnp.float32
    applied, energy = pl.pallas_call(
        functools.partial(kernel, n, scaling),
        out_shape=(
            jax.ShapeDtypeStruct((2, bands, planes), bf16),
            jax.ShapeDtypeStruct((bands,), f32),
        ),
        in_specs=[vmem, smem, anywhere, smem, smem, vmem, vmem, vmem],
        out_specs=(anywhere, vmem),
        scratch_shapes=[
            pltpu.VMEM((2, bands, planes), bf16),
            pltpu.VMEM((atoms * 2 * PROJ, planes), bf16),
            pltpu.VMEM((2, ATOM_BLOCK, planes), f32),
            pltpu.VMEM((radial_coef.shape[0], PROJ, planes), f32),
            pltpu.VMEM((atoms, 2 * PROJ, bands), f32),
            pltpu.VMEM((atoms, 2 * PROJ, bands), bf16),
            pltpu.VMEM((atoms, 2 * PROJ, bands), bf16),
            pltpu.VMEM((atoms, 2 * PROJ, bands), bf16),
            pltpu.VMEM((n, 1, bands), f32),
            pltpu.VMEM((2, bands, planes), bf16),
            pltpu.SemaphoreType.DMA,
            pltpu.SemaphoreType.DMA((2,)),
            pltpu.SemaphoreType.DMA((3,)),
            pltpu.SemaphoreType.DMA((3,)),
        ],
        compiler_params=pltpu.CompilerParams(collective_id=0, has_side_effects=True),
    )(
        miller_index,
        kpoint,
        waves,
        species,
        counts,
        positions,
        radial_coef,
        jnp.transpose(coupling, (2, 1, 0)),
    )
    return applied, energy


def solution(mesh):
    in_specs = (P(None, "ga"), P("kpt"), P(None, "kpt", "ga"), P(), P(), P(), P(), P())
    out_specs = (P(None, "kpt", "ga"), P("kpt"))
    return jax.shard_map(
        on_device, mesh=mesh, in_specs=in_specs, out_specs=out_specs, check_vma=False
    )
```

```python
import functools
import math

import jax
import jax.numpy as jnp
import numpy as np
from jax import lax
from jax.experimental import pallas as pl
from jax.experimental.pallas import tpu as pltpu
from jax.sharding import PartitionSpec as P

PROJ = 8
MGRID = 64
ATOM_BLOCK = 16


def turn_polynomials(degree=8):
    nodes = 0.125 * (1.0 + np.cos(np.pi * (np.arange(200) + 0.5) / 200))
    root = np.sqrt(nodes)
    sine = np.polynomial.Chebyshev.fit(nodes, np.sin(2 * np.pi * root) / root, degree, domain=[0, 0.25])
    cosine = np.polynomial.Chebyshev.fit(nodes, np.cos(2 * np.pi * root), degree, domain=[0, 0.25])
    kind = np.polynomial.Polynomial
    return [[float(c) for c in p.convert(kind=kind).coef] for p in (sine, cosine)]


SINE, COSINE = turn_polynomials()


def horner(coefs, x):
    total = coefs[-1]
    for c in coefs[-2::-1]:
        total = total * x + c
    return total


def owners_of(n, atoms):
    if n % 4 == 0 and atoms % (n // 4) == 0:
        return n // 4, 1, 2
    return n, 0, 1


def peers_of(me, n, body):
    if n <= 32:
        order = sorted(range(1, n), key=lambda k: -min(k, n - k))
        for k in order:
            body(lax.rem(me + k, n))
    else:
        lax.fori_loop(1, n, lambda k, c: (body(lax.rem(me + k, n)), c)[1], 0)


def repeat(count, body):
    if count <= 32:
        for k in range(count):
            body(k)
    else:
        lax.fori_loop(0, count, lambda k, c: (body(k), c)[1], 0)


def loop(count, body):
    if count == 1:
        body(0)
    else:
        lax.fori_loop(0, count, lambda i, c: (body(i), c)[1], 0)


def kernel(
    n,
    scaling,
    miller_hbm,
    kpoint_hbm,
    waves_ref,
    species_hbm,
    counts_hbm,
    positions_hbm,
    radial_hbm,
    coupling_hbm,
    out_ref,
    energy_ref,
    vbuf,
    bbuf,
    trig,
    table,
    part,
    send,
    recv,
    wbuf,
    ebuf,
    tally,
    wave_sem,
    send_sems,
    recv_sems,
    miller_ref,
    kpoint_ref,
    species_ref,
    counts_ref,
    positions_ref,
    radial_ref,
    coupling_ref,
    load_sems,
):
    me = lax.axis_index("ga")
    atoms = coupling_hbm.shape[2]
    q, base, stride = owners_of(n, atoms)
    own = atoms // q
    rank = (me - base) // stride
    is_owner = (me >= base) & (rank < q) & (lax.rem(me - base + n * stride, stride) == 0)
    mine_rank = jnp.clip(rank, 0, q - 1)
    bands = waves_ref.shape[1]
    planes = waves_ref.shape[2]
    species_n, _, terms = radial_hbm.shape
    f32 = jnp.float32

    pairs = (
        (miller_hbm, miller_ref),
        (kpoint_hbm, kpoint_ref),
        (species_hbm, species_ref),
        (counts_hbm, counts_ref),
        (positions_hbm, positions_ref),
        (radial_hbm, radial_ref),
        (coupling_hbm, coupling_ref),
    )
    loads = [pltpu.make_async_copy(a, b, load_sems.at[i]) for i, (a, b) in enumerate(pairs)]
    for load in loads:
        load.start()
    wave_copy = pltpu.make_async_copy(waves_ref, vbuf, wave_sem)
    wave_copy.start()
    barrier = pltpu.get_barrier_semaphore()

    def greet(peer):
        pl.semaphore_signal(
            barrier, inc=1, device_id={"ga": peer}, device_id_type=pl.DeviceIdType.MESH
        )

    peers_of(me, n, greet)

    for load in loads:
        load.wait()
    millers = [miller_ref[c : c + 1, :].astype(f32) for c in range(3)]
    shifted = [millers[c] + kpoint_ref[c] for c in range(3)]
    squared = shifted[0] * shifted[0] + shifted[1] * shifted[1] + shifted[2] * shifted[2]
    row = lax.broadcasted_iota(jnp.int32, (PROJ, planes), 0)
    inverse = 1.0 / jnp.sqrt(squared + 1.0)
    kind = lax.rem(row, 4)
    angular = jnp.full((PROJ, planes), scaling, f32)
    for c in range(3):
        angular = jnp.where(kind == c + 1, shifted[c] * inverse * scaling, angular)
    sums = [jnp.zeros((PROJ, planes), f32) for _ in range(species_n)]
    coefs = [radial_ref[s] for s in range(species_n)]
    for r in range(terms):
        width = float(np.float32(0.001) * np.float32(1.5) ** np.float32(r))
        basis = jnp.exp(-width * squared)
        for s in range(species_n):
            sums[s] = sums[s] + coefs[s][:, r : r + 1] * basis
    for s in range(species_n):
        table[s] = sums[s] * angular

    def build(block):
        first = block * ATOM_BLOCK
        diagonal = lax.broadcasted_iota(jnp.int32, (ATOM_BLOCK, atoms), 0) + first
        diagonal = diagonal == lax.broadcasted_iota(jnp.int32, (ATOM_BLOCK, atoms), 1)
        winding = jnp.zeros((ATOM_BLOCK, planes), f32)
        offset = jnp.zeros((ATOM_BLOCK, 1), f32)
        for c in range(3):
            places = positions_ref[c : c + 1, :].astype(f32)
            column = jnp.sum(jnp.where(diagonal, places, 0.0), axis=1, keepdims=True)
            winding = winding + column * millers[c]
            offset = offset + column * kpoint_ref[c]
        winding = winding - MGRID * jnp.floor(winding * (1.0 / MGRID))
        turns = (winding + offset) * (1.0 / MGRID)
        turns = turns - jnp.floor(turns + 0.5)
        square = turns * turns
        trig[0] = horner(COSINE, square)
        trig[1] = -(turns * horner(SINE, square))
        for a in range(ATOM_BLOCK):
            live = row < counts_ref[first + a]
            amplitude = jnp.where(live, table[species_ref[first + a]], 0.0)
            both = jnp.concatenate(
                [amplitude * trig[0, a : a + 1, :], amplitude * trig[1, a : a + 1, :]], axis=0
            )
            at = (first + a) * (2 * PROJ)
            if not isinstance(at, int):
                at = pl.multiple_of(at, 2 * PROJ)
            bbuf[pl.ds(at, 2 * PROJ), :] = both.astype(bbuf.dtype)

    loop(atoms // ATOM_BLOCK, build)
    wave_copy.wait()
    height = ATOM_BLOCK * 2 * PROJ

    def intersect(block):
        at = block * height
        if not isinstance(at, int):
            at = pl.multiple_of(at, height)
        product = lax.dot_general(
            bbuf[pl.ds(at, height), :],
            vbuf[...].reshape(2 * bands, planes),
            (((1,), (1,)), ((), ())),
            preferred_element_type=f32,
        )
        product = product.reshape(ATOM_BLOCK, 2, PROJ, 2 * bands)
        over_re = product[:, 0, :, :bands] + product[:, 1, :, bands:]
        over_im = product[:, 0, :, bands:] - product[:, 1, :, :bands]
        over = jnp.concatenate([over_re, over_im], axis=1)
        part[pl.ds(block * ATOM_BLOCK, ATOM_BLOCK)] = over
        send[pl.ds(block * ATOM_BLOCK, ATOM_BLOCK)] = over.astype(send.dtype)

    loop(atoms // ATOM_BLOCK, intersect)
    pl.semaphore_wait(barrier, n - 1)

    def many_of(ref, count, sem):
        view = ref.at[pl.ds(0, count)]
        return pltpu.make_async_copy(view, view, sem)

    def scatter(o):
        peer = base + o * stride

        @pl.when(peer != me)
        def _():
            pltpu.make_async_remote_copy(
                src_ref=send.at[pl.ds(o * own, own)],
                dst_ref=recv.at[me],
                send_sem=send_sems.at[0],
                recv_sem=recv_sems.at[0],
                device_id={"ga": peer},
                device_id_type=pl.DeviceIdType.MESH,
            ).start()

    repeat(q, scatter)

    @pl.when(is_owner)
    def _():
        recv[me] = jnp.zeros((own, 2 * PROJ, bands), recv.dtype)
        columns = []
        for k in range(own):
            mine = lax.broadcasted_iota(jnp.int32, (PROJ, atoms), 1) == mine_rank * own + k
            columns.append(
                [
                    jnp.broadcast_to(
                        jnp.sum(jnp.where(mine, coupling_ref[j], 0.0), axis=1, keepdims=True),
                        (PROJ, bands),
                    )
                    for j in range(PROJ)
                ]
            )
        many_of(recv, n - 1, recv_sems.at[0]).wait()
        energy = jnp.zeros((1, bands), f32)
        for k in range(own):
            over = part[mine_rank * own + k]
            for p in range(n):
                over = over + recv[p, k].astype(f32)
            weighted = []
            for half in range(2):
                piece = over[half * PROJ : (half + 1) * PROJ]
                total = columns[k][0] * piece[0:1]
                for j in range(1, PROJ):
                    total = total + columns[k][j] * piece[j : j + 1]
                energy = energy + jnp.sum(total * piece, axis=0, keepdims=True)
                weighted.append(total)
            wbuf[mine_rank, k] = jnp.concatenate(weighted, axis=0).astype(wbuf.dtype)
        ebuf[mine_rank] = energy

        def spread(buffer, index):
            def copy(peer):
                pltpu.make_async_remote_copy(
                    src_ref=buffer.at[mine_rank],
                    dst_ref=buffer.at[mine_rank],
                    send_sem=send_sems.at[index],
                    recv_sem=recv_sems.at[index],
                    device_id={"ga": peer},
                    device_id_type=pl.DeviceIdType.MESH,
                ).start()

            return copy

        peers_of(me, n, spread(wbuf, 1))
        peers_of(me, n, spread(ebuf, 2))
        many_of(send, (q - 1) * own, send_sems.at[0]).wait()
        if q > 1:
            many_of(wbuf, q - 1, recv_sems.at[1]).wait()

    @pl.when(jnp.logical_not(is_owner))
    def _():
        many_of(send, q * own, send_sems.at[0]).wait()
        many_of(wbuf, q, recv_sems.at[1]).wait()

    weights = wbuf[...].reshape(atoms, 2 * PROJ, bands).astype(f32)
    upper, lower = weights[:, :PROJ], weights[:, PROJ:]
    halves = (
        jnp.concatenate([upper, -lower], axis=1),
        jnp.concatenate([lower, upper], axis=1),
    )
    for half in range(2):
        matrix = halves[half].astype(bbuf.dtype).reshape(atoms * 2 * PROJ, bands)
        out_ref[half] = lax.dot_general(
            matrix, bbuf[...], (((0,), (0,)), ((), ())), preferred_element_type=f32
        ).astype(out_ref.dtype)

    @pl.when(is_owner)
    def _():
        if q > 1:
            many_of(ebuf, q - 1, recv_sems.at[2]).wait()

    @pl.when(jnp.logical_not(is_owner))
    def _():
        many_of(ebuf, q, recv_sems.at[2]).wait()

    energy_ref[...] = jnp.sum(ebuf[...], axis=(0, 1)) / (atoms * PROJ)

    @pl.when(is_owner)
    def _():
        for index, buffer in ((1, recv), (2, tally)):
            many_of(buffer, n - 1, send_sems.at[index]).wait()


def on_device(miller_index, kpoint, waves, species, counts, positions, radial_coef, coupling):
    n = lax.axis_size("ga")
    _, bands, planes = waves.shape
    atoms = coupling.shape[0]
    scaling = 1.0 / math.sqrt(planes * n)
    q = owners_of(n, atoms)[0]
    own = atoms // q
    vmem = pl.BlockSpec(memory_space=pltpu.VMEM)
    smem = pl.BlockSpec(memory_space=pltpu.SMEM)
    anywhere = pl.BlockSpec(memory_space=pl.ANY)
    bf16, f32 = jnp.bfloat16, jnp.float32
    applied, energy = pl.pallas_call(
        functools.partial(kernel, n, scaling),
        out_shape=(
            pltpu.VMEM((2, bands, planes), bf16),
            pltpu.VMEM((bands,), f32),
        ),
        in_specs=[anywhere] * 8,
        out_specs=(vmem, vmem),
        scratch_shapes=[
            pltpu.VMEM((2, bands, planes), bf16),
            pltpu.VMEM((atoms * 2 * PROJ, planes), bf16),
            pltpu.VMEM((2, ATOM_BLOCK, planes), f32),
            pltpu.VMEM((radial_coef.shape[0], PROJ, planes), f32),
            pltpu.VMEM((atoms, 2 * PROJ, bands), f32),
            pltpu.VMEM((atoms, 2 * PROJ, bands), bf16),
            pltpu.VMEM((n, own, 2 * PROJ, bands), bf16),
            pltpu.VMEM((q, own, 2 * PROJ, bands), bf16),
            pltpu.VMEM((q, 1, bands), f32),
            pltpu.VMEM((n, 1, bands), f32),
            pltpu.SemaphoreType.DMA,
            pltpu.SemaphoreType.DMA((3,)),
            pltpu.SemaphoreType.DMA((3,)),
            pltpu.VMEM(miller_index.shape, jnp.int32),
            pltpu.SMEM(kpoint.shape, f32),
            pltpu.SMEM(species.shape, jnp.int32),
            pltpu.SMEM(counts.shape, jnp.int32),
            pltpu.VMEM(positions.shape, jnp.int32),
            pltpu.VMEM(radial_coef.shape, f32),
            pltpu.VMEM((PROJ, PROJ, atoms), f32),
            pltpu.SemaphoreType.DMA((7,)),
        ],
        compiler_params=pltpu.CompilerParams(collective_id=0, has_side_effects=True),
    )(
        miller_index,
        kpoint,
        waves,
        species,
        counts,
        positions,
        radial_coef,
        jnp.transpose(coupling, (1, 2, 0)),
    )
    return applied, energy


def solution(mesh):
    in_specs = (P(None, "ga"), P("kpt"), P(None, "kpt", "ga"), P(), P(), P(), P(), P())
    out_specs = (P(None, "kpt", "ga"), P("kpt"))
    return jax.shard_map(
        on_device, mesh=mesh, in_specs=in_specs, out_specs=out_specs, check_vma=False
    )
```

```python
import functools
import math

import jax
import jax.numpy as jnp
import numpy as np
from jax import lax
from jax.experimental import pallas as pl
from jax.experimental.pallas import tpu as pltpu
from jax.sharding import PartitionSpec as P

PROJ = 8
MGRID = 64
SPLIT = 2
ATOM_BLOCK = 8


def turn_polynomials(degree=8):
    nodes = 0.125 * (1.0 + np.cos(np.pi * (np.arange(200) + 0.5) / 200))
    root = np.sqrt(nodes)
    sine = np.polynomial.Chebyshev.fit(nodes, np.sin(2 * np.pi * root) / root, degree, domain=[0, 0.25])
    cosine = np.polynomial.Chebyshev.fit(nodes, np.cos(2 * np.pi * root), degree, domain=[0, 0.25])
    kind = np.polynomial.Polynomial
    return [[float(c) for c in p.convert(kind=kind).coef] for p in (sine, cosine)]


SINE, COSINE = turn_polynomials()


def horner(coefs, x):
    total = coefs[-1]
    for c in coefs[-2::-1]:
        total = total * x + c
    return total


def owners_of(n, atoms):
    if n % 4 == 0 and atoms % (n // 4) == 0:
        return n // 4, 1, 2
    return n, 0, 1


def peers_of(me, n, body):
    def one(peer):
        @pl.when(peer != me)
        def _():
            body(peer)

    if n <= 32:
        for peer in sorted(range(n), key=lambda p: (p // 2 % 2, p)):
            one(peer)
    else:
        repeat(n, one)


def repeat(count, body):
    if count <= 32:
        for k in range(count):
            body(k)
    else:
        lax.fori_loop(0, count, lambda k, c: (body(k), c)[1], 0)


def loop(count, body):
    if count == 1:
        body(0)
    else:
        lax.fori_loop(0, count, lambda i, c: (body(i), c)[1], 0)


def kernel(
    n,
    scaling,
    miller_hbm,
    kpoint_hbm,
    waves_ref,
    species_hbm,
    counts_hbm,
    positions_hbm,
    radial_hbm,
    coupling_hbm,
    out_ref,
    energy_ref,
    vbuf,
    bbuf,
    trig,
    table,
    part,
    send,
    recv,
    wbuf,
    ebuf,
    tally,
    wave_sem,
    send_sems,
    recv_sems,
    miller_ref,
    kpoint_ref,
    species_ref,
    counts_ref,
    positions_ref,
    radial_ref,
    coupling_ref,
    load_sems,
):
    me = lax.axis_index("ga")
    atoms = coupling_hbm.shape[2]
    q, base, stride = owners_of(n, atoms)
    own = atoms // q
    rank = (me - base) // stride
    is_owner = (me >= base) & (rank < q) & (lax.rem(me - base + n * stride, stride) == 0)
    mine_rank = jnp.clip(rank, 0, q - 1)
    halves_n = recv.shape[0]
    share = own // halves_n
    bands = waves_ref.shape[1]
    planes = waves_ref.shape[2]
    species_n, _, terms = radial_hbm.shape
    f32 = jnp.float32

    pairs = (
        (miller_hbm, miller_ref),
        (kpoint_hbm, kpoint_ref),
        (species_hbm, species_ref),
        (counts_hbm, counts_ref),
        (positions_hbm, positions_ref),
        (radial_hbm, radial_ref),
        (coupling_hbm, coupling_ref),
    )
    loads = [pltpu.make_async_copy(a, b, load_sems.at[i]) for i, (a, b) in enumerate(pairs)]
    for load in loads:
        load.start()
    wave_copy = pltpu.make_async_copy(waves_ref, vbuf, wave_sem)
    wave_copy.start()
    barrier = pltpu.get_barrier_semaphore()

    def greet(peer):
        pl.semaphore_signal(
            barrier, inc=1, device_id={"ga": peer}, device_id_type=pl.DeviceIdType.MESH
        )

    peers_of(me, n, greet)

    for load in loads:
        load.wait()
    millers = [miller_ref[c : c + 1, :].astype(f32) for c in range(3)]
    shifted = [millers[c] + kpoint_ref[c] for c in range(3)]
    squared = shifted[0] * shifted[0] + shifted[1] * shifted[1] + shifted[2] * shifted[2]
    row = lax.broadcasted_iota(jnp.int32, (PROJ, planes), 0)
    inverse = 1.0 / jnp.sqrt(squared + 1.0)
    kind = lax.rem(row, 4)
    angular = jnp.full((PROJ, planes), scaling, f32)
    for c in range(3):
        angular = jnp.where(kind == c + 1, shifted[c] * inverse * scaling, angular)
    sums = [jnp.zeros((PROJ, planes), f32) for _ in range(species_n)]
    coefs = [radial_ref[s] for s in range(species_n)]
    for r in range(terms):
        width = float(np.float32(0.001) * np.float32(1.5) ** np.float32(r))
        basis = jnp.exp(-width * squared)
        for s in range(species_n):
            sums[s] = sums[s] + coefs[s][:, r : r + 1] * basis
    for s in range(species_n):
        table[s] = sums[s] * angular

    def build(block):
        first = block * ATOM_BLOCK
        diagonal = lax.broadcasted_iota(jnp.int32, (ATOM_BLOCK, atoms), 0) + first
        diagonal = diagonal == lax.broadcasted_iota(jnp.int32, (ATOM_BLOCK, atoms), 1)
        winding = jnp.zeros((ATOM_BLOCK, planes), f32)
        offset = jnp.zeros((ATOM_BLOCK, 1), f32)
        for c in range(3):
            places = positions_ref[c : c + 1, :].astype(f32)
            column = jnp.sum(jnp.where(diagonal, places, 0.0), axis=1, keepdims=True)
            winding = winding + column * millers[c]
            offset = offset + column * kpoint_ref[c]
        winding = winding - MGRID * jnp.floor(winding * (1.0 / MGRID))
        turns = (winding + offset) * (1.0 / MGRID)
        turns = turns - jnp.floor(turns + 0.5)
        square = turns * turns
        trig[0] = horner(COSINE, square)
        trig[1] = -(turns * horner(SINE, square))
        for a in range(ATOM_BLOCK):
            live = row < counts_ref[first + a]
            amplitude = jnp.where(live, table[species_ref[first + a]], 0.0)
            both = jnp.concatenate(
                [amplitude * trig[0, a : a + 1, :], amplitude * trig[1, a : a + 1, :]], axis=0
            )
            at = (first + a) * (2 * PROJ)
            if not isinstance(at, int):
                at = pl.multiple_of(at, 2 * PROJ)
            bbuf[pl.ds(at, 2 * PROJ), :] = both.astype(bbuf.dtype)

    height = ATOM_BLOCK * 2 * PROJ

    def intersect(block):
        at = block * height
        if not isinstance(at, int):
            at = pl.multiple_of(at, height)
        product = lax.dot_general(
            bbuf[pl.ds(at, height), :],
            vbuf[...].reshape(2 * bands, planes),
            (((1,), (1,)), ((), ())),
            preferred_element_type=f32,
        )
        product = product.reshape(ATOM_BLOCK, 2, PROJ, 2 * bands)
        over_re = product[:, 0, :, :bands] + product[:, 1, :, bands:]
        over_im = product[:, 0, :, bands:] - product[:, 1, :, :bands]
        over = jnp.concatenate([over_re, over_im], axis=1)
        part[pl.ds(block * ATOM_BLOCK, ATOM_BLOCK)] = over
        send[pl.ds(block * ATOM_BLOCK, ATOM_BLOCK)] = over.astype(send.dtype)


    def many_of(ref, count, sem):
        view = ref.at[pl.ds(0, count)]
        return pltpu.make_async_copy(view, view, sem)

    def scatter(h, o):
        peer = base + o * stride

        @pl.when(peer != me)
        def _():
            pltpu.make_async_remote_copy(
                src_ref=send.at[pl.ds(h * (atoms // halves_n) + o * share, share)],
                dst_ref=recv.at[h, me],
                send_sem=send_sems.at[0],
                recv_sem=recv_sems.at[h],
                device_id={"ga": peer},
                device_id_type=pl.DeviceIdType.MESH,
            ).start()

    blocks = atoms // ATOM_BLOCK
    if blocks == halves_n:
        for h in range(halves_n):
            build(h)
            if h == 0:
                wave_copy.wait()
            intersect(h)
            if h == 0:
                pl.semaphore_wait(barrier, n - 1)
            repeat(q, functools.partial(scatter, h))
    else:
        loop(blocks, build)
        wave_copy.wait()
        loop(blocks, intersect)
        pl.semaphore_wait(barrier, n - 1)
        for h in range(halves_n):
            repeat(q, functools.partial(scatter, h))

    @pl.when(is_owner)
    def _():
        columns = []
        for h in range(halves_n):
            recv[h, me] = jnp.zeros((share, 2 * PROJ, bands), recv.dtype)
        for h in range(halves_n):
            for k in range(share):
                atom = h * (atoms // halves_n) + mine_rank * share + k
                mine = lax.broadcasted_iota(jnp.int32, (PROJ, atoms), 1) == atom
                columns.append(
                    [
                        jnp.broadcast_to(
                            jnp.sum(jnp.where(mine, coupling_ref[j], 0.0), axis=1, keepdims=True),
                            (PROJ, bands),
                        )
                        for j in range(PROJ)
                    ]
                )

        def spread(source, target, send_sem, recv_sem):
            def copy(peer):
                pltpu.make_async_remote_copy(
                    src_ref=source,
                    dst_ref=target,
                    send_sem=send_sem,
                    recv_sem=recv_sem,
                    device_id={"ga": peer},
                    device_id_type=pl.DeviceIdType.MESH,
                ).start()

            return copy

        energy = jnp.zeros((1, bands), f32)
        for h in range(halves_n):
            many_of(recv.at[h], n - 1, recv_sems.at[h]).wait()
            for k in range(share):
                over = part[h * (atoms // halves_n) + mine_rank * share + k]
                for p in range(n):
                    over = over + recv[h, p, k].astype(f32)
                weighted = []
                for half in range(2):
                    piece = over[half * PROJ : (half + 1) * PROJ]
                    total = columns[h * share + k][0] * piece[0:1]
                    for j in range(1, PROJ):
                        total = total + columns[h * share + k][j] * piece[j : j + 1]
                    energy = energy + jnp.sum(total * piece, axis=0, keepdims=True)
                    weighted.append(total)
                wbuf[h, mine_rank, k] = jnp.concatenate(weighted, axis=0).astype(wbuf.dtype)
            mine_w = wbuf.at[h, mine_rank]
            peers_of(
                me, n, spread(mine_w, mine_w, send_sems.at[1 + h], recv_sems.at[halves_n + h])
            )
        ebuf[mine_rank] = energy
        mine_e = ebuf.at[mine_rank]
        peers_of(
            me,
            n,
            spread(mine_e, mine_e, send_sems.at[1 + halves_n], recv_sems.at[2 * halves_n]),
        )
        many_of(send, (q - 1) * own, send_sems.at[0]).wait()
        if q > 1:
            for h in range(halves_n):
                many_of(wbuf.at[h], q - 1, recv_sems.at[halves_n + h]).wait()

    @pl.when(jnp.logical_not(is_owner))
    def _():
        many_of(send, q * own, send_sems.at[0]).wait()
        for h in range(halves_n):
            many_of(wbuf.at[h], q, recv_sems.at[halves_n + h]).wait()

    weights = wbuf[...].reshape(atoms, 2 * PROJ, bands).astype(f32)
    upper, lower = weights[:, :PROJ], weights[:, PROJ:]
    halves = (
        jnp.concatenate([upper, -lower], axis=1),
        jnp.concatenate([lower, upper], axis=1),
    )
    for half in range(2):
        matrix = halves[half].astype(bbuf.dtype).reshape(atoms * 2 * PROJ, bands)
        out_ref[half] = lax.dot_general(
            matrix, bbuf[...], (((0,), (0,)), ((), ())), preferred_element_type=f32
        ).astype(out_ref.dtype)

    @pl.when(is_owner)
    def _():
        if q > 1:
            many_of(ebuf, q - 1, recv_sems.at[2 * halves_n]).wait()

    @pl.when(jnp.logical_not(is_owner))
    def _():
        many_of(ebuf, q, recv_sems.at[2 * halves_n]).wait()

    energy_ref[...] = jnp.sum(ebuf[...], axis=(0, 1)) / (atoms * PROJ)

    @pl.when(is_owner)
    def _():
        for h in range(halves_n):
            many_of(recv.at[h], n - 1, send_sems.at[1 + h]).wait()
        many_of(tally, n - 1, send_sems.at[1 + halves_n]).wait()


def on_device(miller_index, kpoint, waves, species, counts, positions, radial_coef, coupling):
    n = lax.axis_size("ga")
    _, bands, planes = waves.shape
    atoms = coupling.shape[0]
    scaling = 1.0 / math.sqrt(planes * n)
    q = owners_of(n, atoms)[0]
    own = atoms // q
    halves_n = SPLIT if own % SPLIT == 0 else 1
    vmem = pl.BlockSpec(memory_space=pltpu.VMEM)
    smem = pl.BlockSpec(memory_space=pltpu.SMEM)
    anywhere = pl.BlockSpec(memory_space=pl.ANY)
    bf16, f32 = jnp.bfloat16, jnp.float32
    applied, energy = pl.pallas_call(
        functools.partial(kernel, n, scaling),
        out_shape=(
            pltpu.VMEM((2, bands, planes), bf16),
            pltpu.VMEM((bands,), f32),
        ),
        in_specs=[anywhere] * 8,
        out_specs=(vmem, vmem),
        scratch_shapes=[
            pltpu.VMEM((2, bands, planes), bf16),
            pltpu.VMEM((atoms * 2 * PROJ, planes), bf16),
            pltpu.VMEM((2, ATOM_BLOCK, planes), f32),
            pltpu.VMEM((radial_coef.shape[0], PROJ, planes), f32),
            pltpu.VMEM((atoms, 2 * PROJ, bands), f32),
            pltpu.VMEM((atoms, 2 * PROJ, bands), bf16),
            pltpu.VMEM((halves_n, n, own // halves_n, 2 * PROJ, bands), bf16),
            pltpu.VMEM((halves_n, q, own // halves_n, 2 * PROJ, bands), bf16),
            pltpu.VMEM((q, 1, bands), f32),
            pltpu.VMEM((n, 1, bands), f32),
            pltpu.SemaphoreType.DMA,
            pltpu.SemaphoreType.DMA((2 + halves_n,)),
            pltpu.SemaphoreType.DMA((1 + 2 * halves_n,)),
            pltpu.VMEM(miller_index.shape, jnp.int32),
            pltpu.SMEM(kpoint.shape, f32),
            pltpu.SMEM(species.shape, jnp.int32),
            pltpu.SMEM(counts.shape, jnp.int32),
            pltpu.VMEM(positions.shape, jnp.int32),
            pltpu.VMEM(radial_coef.shape, f32),
            pltpu.VMEM((PROJ, PROJ, atoms), f32),
            pltpu.SemaphoreType.DMA((7,)),
        ],
        compiler_params=pltpu.CompilerParams(collective_id=0, has_side_effects=True),
    )(
        miller_index,
        kpoint,
        waves,
        species,
        counts,
        positions,
        radial_coef,
        jnp.transpose(coupling, (1, 2, 0)),
    )
    return applied, energy


def solution(mesh):
    in_specs = (P(None, "ga"), P("kpt"), P(None, "kpt", "ga"), P(), P(), P(), P(), P())
    out_specs = (P(None, "kpt", "ga"), P("kpt"))
    return jax.shard_map(
        on_device, mesh=mesh, in_specs=in_specs, out_specs=out_specs, check_vma=False
    )
```
